32 devices in a mesh: seq: 8 (over z, y), tp: 4 (over x, core).
Axes of the slice: x: 2, y: 2, z: 4, core: 2. Of those that a mesh axis runs over, the one named last changes fastest.
Arguments:
- tokens: bfloat16 [4096, 2048], P('seq'), may hold values from -16 to 16
- forget: float32 [4096, 32], P('seq', 'tp'), may hold values from -5 to 0, as said below
- attn_gain: float32 [2048], replicated, may hold values from 0.1 to 1.9
- projections: bfloat16 [3, 2048, 2048], P(None, None, 'tp'), may hold values from -0.125 to 0.125
- out_weight: bfloat16 [2048, 2048], P('tp'), may hold values from -0.125 to 0.125
- ffn_gain: float32 [2048], replicated, may hold values from 0.1 to 1.9
- expand_weight: bfloat16 [2, 2048, 4096], P(None, None, 'tp'), may hold values from -0.125 to 0.125
- down_weight: bfloat16 [4096, 2048], P('tp'), may hold values from -0.09375 to 0.09375
Outputs:
- output: bfloat16 [4096, 2048], P('seq')
The draws below stay inside these ranges and needn't reach their ends.
Inputs may be any that keep to these rules, and one draw needn't show every extreme that they name: forget is never positive.
All inputs are finite; a program needn't handle non-finite values.
Results may differ from the reference program's by a relative error of at most 0.011.
Values may be sent and summed in bfloat16 or wider, within the bound.
No kernel may reach another device: no remote copies, remote signals or barrier semaphores. Data moves between devices by JAX's collectives and lax.ppermute only.
A program may use at most 128 MiB of HBM per device.

```python
import math
import jax
import jax.numpy as jnp
from jax import lax

D = 2048
HEAD_TOTAL = 32
DH = 64
FF = 4096
TOK_DEV = 512
SEQUENCE_TOKENS = 4096


def draw_tokens(key, part):
    random_keys = jax.random.split(key, 3)
    noise = jax.random.normal(random_keys[0], (SEQUENCE_TOKENS, D), jnp.float32)
    row_scale = jnp.exp(jax.random.uniform(random_keys[1], (SEQUENCE_TOKENS, 1), jnp.float32, jnp.log(0.3), jnp.log(3.0)))
    column_scale = jnp.exp(jax.random.uniform(random_keys[2], (1, D), jnp.float32, jnp.log(0.3), jnp.log(3.0)))
    return jnp.clip(noise * row_scale * column_scale, -16.0, 16.0).astype(jnp.bfloat16)


def draw_forget(key, part):
    random_keys = jax.random.split(key, 7)
    slow_share = 0.5
    is_slow = jax.random.uniform(random_keys[0], (HEAD_TOTAL,), jnp.float32) < slow_share
    slow_rate = jax.random.uniform(random_keys[1], (HEAD_TOTAL,), jnp.float32, 0.2, 0.6) / SEQUENCE_TOKENS
    fast_rate = jnp.exp(jax.random.uniform(random_keys[2], (HEAD_TOTAL,), jnp.float32, jnp.log(10.0), jnp.log(16.0))) / TOK_DEV
    base_rate = jnp.where(is_slow, slow_rate, fast_rate)
    block_count = SEQUENCE_TOKENS // TOK_DEV
    device_factor = jnp.exp(jax.random.uniform(random_keys[3], (block_count, 1, HEAD_TOTAL), jnp.float32, jnp.log(0.5), jnp.log(2.0)))
    roughness = jax.random.uniform(random_keys[4], (block_count, TOK_DEV, HEAD_TOTAL), jnp.float32, 0.5, 1.5)
    decay_rates = (base_rate * device_factor * roughness).reshape(SEQUENCE_TOKENS, HEAD_TOTAL)
    spike_positions = jax.random.randint(random_keys[5], (2,), 0, SEQUENCE_TOKENS)
    spike_magnitude = jax.random.uniform(random_keys[6], (2, HEAD_TOTAL), jnp.float32, 0.22, 0.69)
    spike_flags = (jnp.arange(SEQUENCE_TOKENS)[:, None] == spike_positions[None, :]).astype(jnp.float32)
    spike_values = jnp.dot(spike_flags, spike_magnitude)
    return -(decay_rates + spike_values)


def block_scale(key, extent, shards, least, top_value):
    factor_of, own = 1.0, jax.random.fold_in(key, 6)
    for axis_at, blocks in shards:
        draws = jnp.exp(jax.random.uniform(jax.random.fold_in(own, axis_at), (blocks,), jnp.float32, least / len(shards), top_value / len(shards)))
        factor_of = factor_of * jnp.repeat(draws, extent[axis_at] // blocks).reshape([-1 if axis == axis_at else 1 for axis in range(len(extent))])
    return factor_of


def gaussian(stream_key, shape, width, reach, shards=(), dtype=jnp.bfloat16):
    entries = width * jax.random.normal(stream_key, shape, jnp.float32)
    if shards:
        entries = entries * block_scale(stream_key, shape, shards, -0.22, 0.18)
    return jnp.clip(entries, -reach, reach).astype(dtype)


def setup_inputs(seed: int = 0) -> dict:
    splits = jax.random.split(jax.random.key(seed), 9)
    tokens = draw_tokens(jax.random.fold_in(splits[8], 71), 0)
    forget = draw_forget(jax.random.fold_in(splits[8], 71), 0)
    attn_gain = jnp.clip(1.0 + 0.18 * jax.random.normal(splits[2], (D,), jnp.float32), 0.1, 1.9)
    projections = gaussian(splits[3], (3, D, HEAD_TOTAL * DH), D ** -0.5, 0.125, ((2, 4),))
    out_weight = gaussian(splits[4], (HEAD_TOTAL * DH, D), (HEAD_TOTAL * DH) ** -0.5, 0.125, ((0, 4),))
    ffn_gain = jnp.clip(1.0 + 0.18 * jax.random.normal(splits[5], (D,), jnp.float32), 0.1, 1.9)
    expand_weight = gaussian(splits[6], (2, D, FF), D ** -0.5, 0.125, ((2, 4),))
    down_weight = gaussian(splits[7], (FF, D), FF ** -0.5, 0.09375, ((0, 4),))
    return dict(tokens=tokens, forget=forget, attn_gain=attn_gain, projections=projections, out_weight=out_weight, ffn_gain=ffn_gain, expand_weight=expand_weight, down_weight=down_weight)


norm_epsilon = 1e-05
head_epsilon = 1e-06

def rms_scale(values, gain_vector):
    widened = values.astype(jnp.float32)
    mean_square = lax.optimization_barrier(jnp.mean(widened * widened, axis=-1, keepdims=True))
    return widened * lax.rsqrt(mean_square + norm_epsilon) * gain_vector

def summarize(key_rows, value_rows, forget_rows):
    log_decay = jnp.cumsum(forget_rows, axis=0)
    block_total = log_decay[-1]
    shrink_factors = jnp.exp(block_total[None, :] - log_decay)
    scaled_keys = (key_rows.astype(jnp.float32) * shrink_factors[:, :, None]).astype(jnp.bfloat16)
    block_state = jnp.einsum('shd,she->hde', scaled_keys.astype(jnp.float32), value_rows.astype(jnp.float32), precision=lax.Precision.HIGHEST)
    return (log_decay, block_total, block_state)

def attend_local(query_rows, key_rows, value_rows, log_decay, incoming):
    head_size = query_rows.shape[2]
    score_scale = 1.0 / math.sqrt(head_size)
    query_wide = query_rows.astype(jnp.float32)
    scores = jnp.einsum('thd,shd->hts', query_wide, key_rows.astype(jnp.float32), precision=lax.Precision.HIGHEST) * score_scale
    log_gaps = log_decay.T[:, :, None] - log_decay.T[:, None, :]
    row_order = jnp.arange(query_rows.shape[0])
    causal = (row_order[:, None] >= row_order[None, :])[None]
    local_weights = jnp.where(causal, scores * jnp.exp(jnp.where(causal, log_gaps, 0.0)), 0.0).astype(jnp.bfloat16)
    local_part = jnp.einsum('hts,she->the', local_weights.astype(jnp.float32), value_rows.astype(jnp.float32), precision=lax.Precision.HIGHEST)
    carried = jnp.einsum('thd,hde->the', query_wide, incoming, precision=lax.Precision.HIGHEST)
    attended = local_part + carried * (jnp.exp(log_decay) * score_scale)[:, :, None]
    mean_square = lax.optimization_barrier(jnp.mean(attended * attended, axis=-1, keepdims=True))
    return (attended * lax.rsqrt(mean_square + head_epsilon)).astype(jnp.bfloat16)

def reference(tokens, forget, attn_gain, projections, out_weight, ffn_gain, expand_weight, down_weight):
    normed = rms_scale(tokens, attn_gain).astype(jnp.bfloat16)
    block_count = SEQUENCE_TOKENS // TOK_DEV
    shaped = []
    for which in range(3):
        projected = jnp.dot(normed, projections[which], preferred_element_type=jnp.float32).astype(jnp.bfloat16)
        shaped.append(projected.reshape(block_count, TOK_DEV, HEAD_TOTAL, DH))
    forget_blocks = forget.reshape(block_count, TOK_DEV, HEAD_TOTAL)

    def block_step(incoming, block_data):
        query_rows, key_rows, value_rows, forget_rows = block_data
        log_decay, block_total, block_state = summarize(key_rows, value_rows, forget_rows)
        head_out = attend_local(query_rows, key_rows, value_rows, log_decay, incoming)
        following = jnp.exp(block_total)[:, None, None] * incoming + block_state
        return (following, head_out)
    start_state = jnp.zeros((HEAD_TOTAL, DH, DH), jnp.float32)
    _, head_blocks = lax.scan(block_step, start_state, (shaped[0], shaped[1], shaped[2], forget_blocks))
    head_out = head_blocks.reshape(SEQUENCE_TOKENS, HEAD_TOTAL * DH)
    attn_out = jnp.dot(head_out, out_weight, preferred_element_type=jnp.float32)
    residual = (tokens.astype(jnp.float32) + attn_out).astype(jnp.bfloat16)
    normed_ffn = rms_scale(residual, ffn_gain).astype(jnp.bfloat16)
    gate_proj = jnp.dot(normed_ffn, expand_weight[0], preferred_element_type=jnp.float32)
    up_proj = jnp.dot(normed_ffn, expand_weight[1], preferred_element_type=jnp.float32)
    hidden = (jax.nn.silu(gate_proj) * up_proj).astype(jnp.bfloat16)
    ffn_out = jnp.dot(hidden, down_weight, preferred_element_type=jnp.float32)
    return (residual.astype(jnp.float32) + ffn_out).astype(jnp.bfloat16)
```

```python
import math

import jax
import jax.numpy as jnp
from jax import lax
from jax.sharding import PartitionSpec as P

norm_epsilon = 1e-05
head_epsilon = 1e-06
cores = 2


def rms_scale(values, gain_vector):
    widened = values.astype(jnp.float32)
    mean_square = jnp.mean(widened * widened, axis=-1, keepdims=True)
    return (widened * lax.rsqrt(mean_square + norm_epsilon) * gain_vector).astype(jnp.bfloat16)


def matmul(a, b):
    return jnp.dot(a, b, preferred_element_type=jnp.float32)


def swap_cores(value):
    count = lax.axis_size("tp")
    return lax.ppermute(value, "tp", [(i, i ^ 1) for i in range(count)])


def across_chips(value):
    count = lax.axis_size("tp")
    return lax.ppermute(value, "tp", [(i, (i + cores) % count) for i in range(count)])


def with_seq(value, bit):
    count = lax.axis_size("seq")
    return lax.ppermute(value, "seq", [(i, i ^ bit) for i in range(count)])


def summarize(key_rows, value_rows, forget_rows):
    log_decay = jnp.cumsum(forget_rows, axis=0)
    block_total = log_decay[-1]
    shrink_factors = jnp.exp(block_total[None, :] - log_decay)
    scaled_keys = (key_rows.astype(jnp.float32) * shrink_factors[:, :, None]).astype(jnp.bfloat16)
    block_state = jnp.einsum(
        "shd,she->hde", scaled_keys, value_rows, preferred_element_type=jnp.float32
    )
    return (log_decay, block_total, block_state)


def incoming_state(block_decay, block_state):
    count, mine = lax.axis_size("seq"), lax.axis_index("seq")
    heads, size = block_state.shape[:2]
    lanes = 2 * size
    shape = (heads, size * size // lanes, lanes)
    state = block_state.reshape(shape)
    decay = jnp.broadcast_to(block_decay[:, None, None], (heads, 1, lanes))
    before, before_decay = jnp.zeros_like(state), jnp.ones_like(decay)
    bit = 1
    while bit < count:
        sent = jnp.concatenate([state, decay], axis=1).astype(jnp.bfloat16)
        got = with_seq(sent, bit).astype(jnp.float32)
        got_state, got_decay = got[:, :-1], got[:, -1:]
        later = (mine & bit) != 0
        before = jnp.where(later, before + before_decay * got_state, before)
        before_decay = jnp.where(later, before_decay * got_decay, before_decay)
        state = jnp.where(later, decay * got_state + state, got_decay * state + got_state)
        decay = decay * got_decay
        bit *= 2
    return before.reshape(heads, size, size)


def local_attention(query_rows, key_rows, value_rows, log_decay):
    head_size = query_rows.shape[2]
    score_scale = 1.0 / math.sqrt(head_size)
    scores = (
        jnp.einsum("thd,shd->hts", query_rows, key_rows, preferred_element_type=jnp.float32)
        * score_scale
    )
    log_gaps = log_decay.T[:, :, None] - log_decay.T[:, None, :]
    row_order = jnp.arange(query_rows.shape[0])
    causal = (row_order[:, None] >= row_order[None, :])[None]
    local_weights = jnp.where(
        causal, scores * jnp.exp(jnp.where(causal, log_gaps, 0.0)), 0.0
    ).astype(jnp.bfloat16)
    return jnp.einsum("hts,she->the", local_weights, value_rows, preferred_element_type=jnp.float32)


def finish_heads(query_rows, local_part, log_decay, incoming):
    head_size = query_rows.shape[2]
    score_scale = 1.0 / math.sqrt(head_size)
    carried = jnp.einsum(
        "thd,hde->the",
        query_rows,
        incoming.astype(jnp.bfloat16),
        preferred_element_type=jnp.float32,
    )
    attended = local_part + carried * (jnp.exp(log_decay) * score_scale)[:, :, None]
    mean_square = jnp.mean(attended * attended, axis=-1, keepdims=True)
    head_out = (attended * lax.rsqrt(mean_square + head_epsilon)).astype(jnp.bfloat16)
    return head_out.reshape(query_rows.shape[0], -1)


def local(tokens, forget, attn_gain, projections, out_weight, ffn_gain, expand_weight, down_weight):
    row_count, width = tokens.shape
    head_count = forget.shape[1]
    head_size = projections.shape[2] // head_count
    chips = lax.axis_size("tp") // cores
    half = row_count // cores
    core = lax.axis_index("tp") % cores
    parity = lax.axis_index("seq") % 2

    out_share = out_weight.shape[0] // 2
    chip_out = [jnp.concatenate([out_weight, swap_cores(out_weight)], axis=0)]
    far = lax.dynamic_slice_in_dim(out_weight, parity * out_share, out_share, 0)
    for _ in range(chips - 1):
        far = across_chips(far)
        other = with_seq(far, 1)
        first = jnp.where(parity == 0, far, other)
        second = jnp.where(parity == 0, other, far)
        whole = jnp.concatenate([first, second], axis=0)
        chip_out.append(jnp.concatenate([whole, swap_cores(whole)], axis=0))
    expand_pair = (expand_weight, swap_cores(expand_weight))
    down_pair = (down_weight, swap_cores(down_weight))

    normed = rms_scale(tokens, attn_gain)
    shaped = []
    for which in range(3):
        projected = matmul(normed, projections[which]).astype(jnp.bfloat16)
        shaped.append(projected.reshape(row_count, head_count, head_size))
    query_rows, key_rows, value_rows = shaped
    log_decay, block_total, block_state = summarize(key_rows, value_rows, forget)
    incoming = incoming_state(jnp.exp(block_total), block_state)
    local_part = local_attention(query_rows, key_rows, value_rows, log_decay)
    head_out = finish_heads(query_rows, local_part, log_decay, incoming)

    kept = lax.dynamic_slice_in_dim(head_out, core * half, half, 0)
    given = lax.dynamic_slice_in_dim(head_out, (1 - core) * half, half, 0)
    heads = jnp.concatenate([kept, swap_cores(given)], axis=1)
    attn_sum = matmul(heads, chip_out[0])
    for hop in range(1, chips):
        heads = across_chips(heads)
        attn_sum = attn_sum + matmul(heads, chip_out[hop])
    own_tokens = lax.dynamic_slice_in_dim(tokens, core * half, half, 0)
    residual = (own_tokens.astype(jnp.float32) + attn_sum).astype(jnp.bfloat16)
    normed_ffn = rms_scale(residual, ffn_gain)
    hidden = []
    for weight in expand_pair:
        gate_proj = matmul(normed_ffn, weight[0])
        up_proj = matmul(normed_ffn, weight[1])
        hidden.append((jax.nn.silu(gate_proj) * up_proj).astype(jnp.bfloat16))
    pieces = 4
    span = width // pieces
    finished = []
    for piece in range(pieces):
        columns = slice(piece * span, (piece + 1) * span)
        partial = matmul(hidden[0], down_pair[0][:, columns])
        partial = (partial + matmul(hidden[1], down_pair[1][:, columns])).astype(jnp.bfloat16)
        total, moving = partial.astype(jnp.float32), partial
        for hop in range(1, chips):
            moving = across_chips(moving)
            total = total + moving.astype(jnp.float32)
        done = (residual[:, columns].astype(jnp.float32) + total).astype(jnp.bfloat16)
        finished.append(done)
    mine = jnp.concatenate(finished, axis=1)
    theirs = swap_cores(mine)
    upper = jnp.where(core == 0, mine, theirs)
    lower = jnp.where(core == 0, theirs, mine)
    return jnp.concatenate([upper, lower], axis=0)


def solution(mesh):
    placed = (
        P("seq", None),
        P("seq", "tp"),
        P(),
        P(None, None, "tp"),
        P("tp", None),
        P(),
        P(None, None, "tp"),
        P("tp", None),
    )
    return jax.shard_map(
        local, mesh=mesh, in_specs=placed, out_specs=P("seq", None), check_vma=False
    )
```

```python
import functools
import math

import jax
import jax.numpy as jnp
from jax import lax
from jax.experimental import pallas as pl
from jax.experimental.pallas import tpu as pltpu
from jax.sharding import PartitionSpec as P

norm_epsilon = 1e-05
head_epsilon = 1e-06
cores = 2
log2e = 1.4426950408889634

f32, bf16 = jnp.float32, jnp.bfloat16


vmem = pl.BlockSpec(memory_space=pltpu.VMEM)
smem = pl.BlockSpec(memory_space=pltpu.SMEM)
hbm = pl.BlockSpec(memory_space=pltpu.HBM)


def cost(flops):
    return pl.CostEstimate(flops=flops, bytes_accessed=0, transcendentals=0)


def room(mebibytes):
    return pltpu.CompilerParams(vmem_limit_bytes=mebibytes << 20)


def scalar(value):
    return value.astype(jnp.int32).reshape(1)


def iota(shape, axis):
    return lax.broadcasted_iota(jnp.int32, shape, axis)


def dot(a, b):
    return jnp.dot(a, b, preferred_element_type=f32)


def contract(a, b, dim_a, dim_b):
    return lax.dot_general(a, b, (((dim_a,), (dim_b,)), ((), ())), preferred_element_type=f32)


def split3(value):
    high = value.astype(bf16)
    rest = value - high.astype(f32)
    middle = rest.astype(bf16)
    return high, middle, (rest - middle.astype(f32)).astype(bf16)


def normalize(rows, gain):
    mean_square = jnp.mean(rows * rows, axis=-1, keepdims=True)
    return (rows * lax.rsqrt(mean_square + norm_epsilon) * gain).astype(bf16)


def spread_heads(sums, size):
    heads = sums.shape[1]
    spread = (iota((heads, heads * size), 1) // size == iota((heads, heads * size), 0)).astype(bf16)
    parts = split3(sums)
    return dot(parts[0], spread) + dot(parts[1], spread) + dot(parts[2], spread)


def swap_cores(value):
    count = lax.axis_size("tp")
    return lax.ppermute(value, "tp", [(i, i ^ 1) for i in range(count)])


def across_chips(value):
    count = lax.axis_size("tp")
    return lax.ppermute(value, "tp", [(i, (i + cores) % count) for i in range(count)])


def with_seq(value, bit):
    count = lax.axis_size("seq")
    return lax.ppermute(value, "seq", [(i, i ^ bit) for i in range(count)])


def cut_kernel(group, source, *refs):
    outs, sems = refs[:-1], refs[-1]
    share = outs[0].shape[1]
    loads = []
    for at, out in enumerate(outs):
        columns = pl.ds(pl.multiple_of((len(outs) * group[0] + at) * share, share), share)
        loads.append(pltpu.make_async_copy(source.at[:, columns], out, sems.at[at]))
    for load in loads:
        load.start()
    for load in loads:
        load.wait()


def cut_columns(group, weight, pieces):
    share = weight.shape[1] // (2 * pieces)
    return pl.pallas_call(
        cut_kernel,
        in_specs=[smem, hbm],
        out_specs=[hbm] * pieces,
        out_shape=[jax.ShapeDtypeStruct((weight.shape[0], share), weight.dtype)] * pieces,
        scratch_shapes=[pltpu.SemaphoreType.DMA((pieces,))],
        compiler_params=room(1),
        cost_estimate=cost(1 << 30),
        name="cut_columns",
    )(scalar(group), weight)


def project_kernel(
    size, tok, gain, forget, weight, keys, values, normed, query_weight, column, row, state, sent, tok_here, weight_here, sems
):
    heads, rows = forget.shape
    parts = 4
    span = rows // parts
    loads = [
        pltpu.make_async_copy(tok.at[pl.ds(p * span, span)], tok_here.at[pl.ds(p * span, span)], sems.at[p])
        for p in range(parts)
    ]
    for which in (1, 2):
        loads.append(pltpu.make_async_copy(weight.at[which], weight_here.at[which - 1], sems.at[parts + which - 1]))
    loads.append(pltpu.make_async_copy(weight.at[0], query_weight, sems.at[parts + 2]))
    for load in loads:
        load.start()

    pieces = split3(forget[...])
    upper = (iota((rows, rows), 0) <= iota((rows, rows), 1)).astype(bf16)
    sums = (dot(pieces[0], upper) + dot(pieces[1], upper) + dot(pieces[2], upper)) * log2e
    row[...] = sums
    by_token = jnp.transpose(sums)
    column[...] = by_token
    grown = spread_heads(by_token, size)
    ends = grown[rows - 1 :, :]
    decays = jnp.exp2(ends)

    for p in range(parts):
        loads[p].wait()
        here = pl.ds(p * span, span)
        normed[here, :] = normalize(tok_here[here, :].astype(f32), gain[...])
    loads[parts].wait()
    keys[...] = dot(normed[...], weight_here[0]).astype(bf16)
    loads[parts + 1].wait()
    values[...] = dot(normed[...], weight_here[1]).astype(bf16)

    lanes = 2 * size
    first = iota((size, lanes), 1) < size
    picked = jnp.zeros((16, lanes), f32)
    for pair in range(heads // 2):
        cut = slice(pair * lanes, (pair + 1) * lanes)
        shrink = jnp.exp2(ends[:, cut] - grown[:, cut])
        scaled = (keys[:, cut].astype(f32) * shrink).astype(bf16)
        both = contract(scaled, values[:, cut], 0, 0)
        compact = jnp.where(first, both[:size], both[size:])
        state[pl.ds(pair * size, size), :] = compact
        sent[pl.ds(pair * size, size), :] = compact.astype(bf16)
        picked = jnp.where(iota((16, lanes), 0) == pair, jnp.broadcast_to(decays[:, cut], (16, lanes)), picked)
    base = heads // 2 * size
    state[pl.ds(base, 16), :] = picked
    sent[pl.ds(base, 16), :] = picked.astype(bf16)
    loads[parts + 2].wait()


def project(tokens, gain, forget, projections, size):
    rows, width = tokens.shape
    heads = forget.shape[1]
    mine = projections.shape[2]
    packed = (heads // 2 * size + 16, 2 * size)
    outs = [
        ((rows, mine), bf16),
        ((rows, mine), bf16),
        ((rows, width), bf16),
        ((width, mine), bf16),
        ((rows, heads), f32),
        ((heads, rows), f32),
        (packed, f32),
        (packed, bf16),
    ]
    return pl.pallas_call(
        functools.partial(project_kernel, size),
        in_specs=[hbm, vmem, vmem, hbm],
        out_specs=[vmem] * len(outs),
        out_shape=[jax.ShapeDtypeStruct(shape, kind) for shape, kind in outs],
        scratch_shapes=[
            pltpu.VMEM((rows, width), bf16),
            pltpu.VMEM((2, width, mine), bf16),
            pltpu.SemaphoreType.DMA((7,)),
        ],
        cost_estimate=cost(4 * rows * width * mine),
        compiler_params=room(24),
        name="project",
    )(tokens, gain.reshape(1, width), forget.T, projections)


def query_kernel(scale, normed, weight, out):
    out[...] = (dot(normed[...], weight[...]).astype(bf16).astype(f32) * scale).astype(bf16)


def queries(normed, weight, size):
    rows, width = normed.shape
    mine = weight.shape[1]
    return pl.pallas_call(
        functools.partial(query_kernel, 1.0 / math.sqrt(size)),
        in_specs=[vmem] * 2,
        out_specs=vmem,
        out_shape=jax.ShapeDtypeStruct((rows, mine), bf16),
        cost_estimate=cost(2 * rows * width * mine),
        compiler_params=room(8),
        name="queries",
    )(normed, weight)


def block_kernel(size, first_pair, pairs, q, k, v, column, row, out):
    rows, lanes = q.shape[0], 2 * size
    span = rows // 2
    below = iota((span, span), 0) >= iota((span, span), 1)
    for at in range(pairs):
        cut = slice((first_pair + at) * lanes, (first_pair + at + 1) * lanes)
        total = [None, None]
        for side in range(2):
            head = 2 * (first_pair + at) + side
            half = (iota((span, lanes), 1) // size) == side
            zero = jnp.zeros((span, lanes), bf16)
            ks = [jnp.where(half, k[pl.ds(b * span, span), cut], zero) for b in range(2)]
            vs = [jnp.where(half, v[pl.ds(b * span, span), cut], zero) for b in range(2)]
            for tb in range(2):
                here = column[pl.ds(tb * span, span), head : head + 1]
                for sb in range(tb + 1):
                    scores = contract(q[pl.ds(tb * span, span), cut], ks[sb], 1, 1)
                    gap = here - row[head : head + 1, pl.ds(sb * span, span)]
                    if sb == tb:
                        gap = jnp.where(below, gap, -jnp.inf)
                    weights = (scores * jnp.exp2(gap)).astype(bf16)
                    part = dot(weights, vs[sb])
                    total[tb] = part if total[tb] is None else total[tb] + part
        for tb in range(2):
            out[pl.ds(tb * span, span), pl.ds(at * lanes, lanes)] = total[tb]


def block_attention(q, k, v, column, row, size, part, parts):
    rows, mine = q.shape
    heads = column.shape[1]
    wide = mine // parts
    first_pair = part * (heads // 2 // parts)
    return pl.pallas_call(
        functools.partial(block_kernel, size, first_pair, heads // 2 // parts),
        in_specs=[vmem] * 5,
        out_specs=vmem,
        out_shape=jax.ShapeDtypeStruct((rows, wide), f32),
        cost_estimate=cost(16 * rows * rows * wide),
        compiler_params=room(10),
    )(q, k, v, column, row)


def combine_kernel(first, size, later, state, before, got, new_state, new_before, sent):
    tail = 16
    body, lanes = state.shape[0] - tail, state.shape[1]
    is_later = later[0] != 0
    rest = pl.ds(body, tail)
    mine_decay, got_decay = state[rest, :], got[rest, :].astype(f32)
    early_decay = jnp.ones((tail, lanes), f32) if first else before[rest, :]
    for pair in range(body // size):
        at = pl.ds(pair * size, size)
        theirs, own = got[at, :].astype(f32), state[at, :]
        prior = jnp.zeros((size, lanes), f32) if first else before[at, :]
        d_mine, d_got, d_early = (x[pair : pair + 1] for x in (mine_decay, got_decay, early_decay))
        fresh = jnp.where(is_later, d_mine * theirs + own, d_got * own + theirs)
        new_state[at, :] = fresh
        sent[at, :] = fresh.astype(bf16)
        new_before[at, :] = jnp.where(is_later, prior + d_early * theirs, prior)
    decay = mine_decay * got_decay
    new_state[rest, :] = decay
    sent[rest, :] = decay.astype(bf16)
    new_before[rest, :] = jnp.where(is_later, early_decay * got_decay, early_decay)


def combine(first, size, later, state, before, got):
    shape = state.shape
    return pl.pallas_call(
        functools.partial(combine_kernel, first, size),
        in_specs=[smem] + [vmem] * 3,
        out_specs=[vmem] * 3,
        out_shape=[
            jax.ShapeDtypeStruct(shape, f32),
            jax.ShapeDtypeStruct(shape, f32),
            jax.ShapeDtypeStruct(shape, bf16),
        ],
        compiler_params=room(2),
        cost_estimate=cost(1 << 28),
        name="combine",
    )(scalar(later), state, before, got)


def incoming_state(state, sent, size):
    count, mine = lax.axis_size("seq"), lax.axis_index("seq")
    before, bit = state, 1
    while bit < count:
        got = with_seq(sent, bit)
        state, before, sent = combine(bit == 1, size, mine & bit, state, before, got)
        bit *= 2
    return before


def heads_kernel(size, parts, half, q, column, before, *refs):
    locals_, out = refs[:parts], refs[parts]
    span, lanes = out.shape[0], 2 * size
    width = q.shape[1] // parts
    here = pl.ds(pl.multiple_of(half[0] * span, span), span)
    ones = (iota((lanes, lanes), 0) // size == iota((lanes, lanes), 1) // size).astype(bf16)
    first = iota((size, lanes), 1) < size
    growth = jnp.exp2(spread_heads(column[here, :], size))
    for pair in range(q.shape[1] // lanes):
        cut = slice(pair * lanes, (pair + 1) * lanes)
        compact = before[pl.ds(pair * size, size), :]
        upper = jnp.where(first, compact, 0.0).astype(bf16)
        under = jnp.where(first, 0.0, compact).astype(bf16)
        block = jnp.concatenate([upper, under], axis=0)
        carried = dot(q[here, cut], block) * growth[:, cut]
        at = pair * lanes % width
        attended = locals_[pair * lanes // width][here, at : at + lanes] + carried
        square = attended * attended
        high = square.astype(bf16)
        low = (square - high.astype(f32)).astype(bf16)
        mean_square = (dot(high, ones) + dot(low, ones)) * (1.0 / size)
        out[:, cut] = (attended * lax.rsqrt(mean_square + head_epsilon)).astype(bf16)


def finish_heads(half, q, column, before, local_parts, size):
    rows, mine = q.shape
    span = rows // cores
    return pl.pallas_call(
        functools.partial(heads_kernel, size, len(local_parts)),
        in_specs=[smem] + [vmem] * (3 + len(local_parts)),
        out_specs=vmem,
        out_shape=jax.ShapeDtypeStruct((span, mine), bf16),
        cost_estimate=cost(span * mine * 2048),
        compiler_params=room(6),
        name="finish_heads",
    )(scalar(half), q, column, before, *local_parts)


def own_heads_kernel(kept, moved, own, partner, expand_own, expand_other, out, own_here, other_here, first, second, sems):
    pairs = ((own, first), (partner, second), (expand_own, own_here), (expand_other, other_here))
    loads = [pltpu.make_async_copy(a, b, sems.at[at]) for at, (a, b) in enumerate(pairs)]
    for load in loads:
        load.start()
    for load in loads[:2]:
        load.wait()
    out[...] = dot(kept[...], first[...]) + dot(moved[...], second[...])
    for load in loads[2:]:
        load.wait()


def project_own_heads(kept, moved, own, partner, expand_own, expand_other):
    rows, depth = kept.shape
    width = own.shape[1]
    staged = jax.ShapeDtypeStruct(expand_own.shape, bf16)
    return pl.pallas_call(
        own_heads_kernel,
        in_specs=[vmem] * 2 + [hbm] * 4,
        out_specs=[vmem] * 3,
        out_shape=[jax.ShapeDtypeStruct((rows, width), f32), staged, staged],
        scratch_shapes=[pltpu.VMEM(own.shape, bf16), pltpu.VMEM(own.shape, bf16), pltpu.SemaphoreType.DMA((4,))],
        cost_estimate=cost(4 * rows * depth * width),
        compiler_params=room(8),
        name="project_own_heads",
    )(kept, moved, own, partner, expand_own, expand_other)


def far_heads_kernel(parity, kept, moved, *refs):
    weights, (sums, out) = refs[:8], refs[8:]
    share = weights[0].shape[1]
    for at in range(4):
        group = parity[0] if at < 2 else 1 - parity[0]
        here = pl.ds(pl.multiple_of((2 * group + at % 2) * share, share), share)
        part = dot(kept[...], weights[2 * at][...]) + dot(moved[...], weights[2 * at + 1][...])
        out[:, here] = sums[:, here] + part


def project_far_heads(parity, kept, moved, weights, sums):
    rows, depth = kept.shape
    width = sums.shape[1]
    return pl.pallas_call(
        far_heads_kernel,
        in_specs=[smem] + [vmem] * 11,
        out_specs=vmem,
        out_shape=jax.ShapeDtypeStruct(sums.shape, f32),
        input_output_aliases={11: 0},
        cost_estimate=cost(4 * rows * depth * width),
        compiler_params=room(12),
        name="project_far_heads",
    )(scalar(parity), kept, moved, *weights, sums)


def residual_kernel(core, tok, sums, gain, residual, normed):
    rows = sums.shape[0]
    here = pl.ds(pl.multiple_of(core[0] * rows, rows), rows)
    total = (tok[here, :].astype(f32) + sums[...]).astype(bf16)
    residual[...] = total
    normed[...] = normalize(total.astype(f32), gain[...])


def add_residual(core, tokens, sums, gain):
    shape = jax.ShapeDtypeStruct(sums.shape, bf16)
    return pl.pallas_call(
        residual_kernel,
        in_specs=[smem] + [vmem] * 3,
        out_specs=[vmem] * 2,
        out_shape=[shape, shape],
        cost_estimate=cost(sums.size * 1024),
        compiler_params=room(10),
        name="add_residual",
    )(scalar(core), tokens, sums, gain.reshape(1, -1))


def expand_kernel(rows_in, own, other, down_own, down_other, out, own_here, other_here, sems):
    pairs = ((down_own, own_here), (down_other, other_here))
    loads = [pltpu.make_async_copy(a, b, sems.at[at]) for at, (a, b) in enumerate(pairs)]
    for load in loads:
        load.start()
    hidden = own.shape[2]
    wide = hidden // 2
    for place, weight in enumerate((own, other)):
        for at in range(0, hidden, wide):
            gate = dot(rows_in[...], weight[0, :, at : at + wide])
            up = dot(rows_in[...], weight[1, :, at : at + wide])
            half_gate = 0.5 * gate
            silu = half_gate * jnp.tanh(half_gate) + half_gate
            out[:, pl.ds(place * hidden + at, wide)] = (silu * up).astype(bf16)
    for load in loads:
        load.wait()


def expand(rows_in, own, other, down_own, down_other):
    rows, width = rows_in.shape
    hidden = own.shape[2]
    staged = jax.ShapeDtypeStruct(down_own.shape, bf16)
    return pl.pallas_call(
        expand_kernel,
        in_specs=[vmem] * 3 + [hbm] * 2,
        out_specs=[vmem] * 3,
        out_shape=[jax.ShapeDtypeStruct((rows, 2 * hidden), bf16), staged, staged],
        scratch_shapes=[pltpu.SemaphoreType.DMA((2,))],
        cost_estimate=cost(8 * rows * width * hidden),
        compiler_params=room(8),
        name="expand",
    )(rows_in, own, other, down_own, down_other)


def down_kernel(start, hidden, own, other, out):
    depth, span = own.shape[0], out.shape[1]
    cut = slice(start, start + span)
    out[...] = (dot(hidden[:, :depth], own[:, cut]) + dot(hidden[:, depth:], other[:, cut])).astype(bf16)


def down(hidden, own, other, start, span):
    rows, depth = hidden.shape
    return pl.pallas_call(
        functools.partial(down_kernel, start),
        in_specs=[vmem] * 3,
        out_specs=vmem,
        out_shape=jax.ShapeDtypeStruct((rows, span), bf16),
        cost_estimate=cost(2 * rows * depth * span),
        compiler_params=room(14),
    )(hidden, own, other)


def add_kernel(start, residual, own, *refs):
    out = refs[-1]
    total = own[...].astype(f32)
    for other in refs[:-1]:
        total = total + other[...].astype(f32)
    out[...] = (residual[:, start : start + out.shape[1]].astype(f32) + total).astype(bf16)


def add_partials(start, residual, own, others):
    return pl.pallas_call(
        functools.partial(add_kernel, start),
        in_specs=[vmem] * (2 + len(others)),
        out_specs=vmem,
        out_shape=jax.ShapeDtypeStruct(own.shape, bf16),
        compiler_params=room(4),
        cost_estimate=cost(1 << 28),
        name="add_partials",
    )(residual, own, *others)


def place_kernel(count, core, *refs):
    pieces, out, sems = refs[: 2 * count], refs[-2], refs[-1]
    rows = pieces[0].shape[0]
    loads, start = [], 0
    for at in range(count):
        span = pieces[2 * at].shape[1]
        for side in range(2):
            here = pl.ds(pl.multiple_of((core[0] if side == 0 else 1 - core[0]) * rows, rows), rows)
            to = out.at[here, pl.ds(start, span)]
            loads.append(pltpu.make_async_copy(pieces[2 * at + side], to, sems.at[2 * at + side]))
        start += span
    for load in loads:
        load.start()
    for load in loads:
        load.wait()


def place(core, mine, theirs, rows):
    pieces = [x for pair in zip(mine, theirs) for x in pair]
    width = sum(x.shape[1] for x in mine)
    return pl.pallas_call(
        functools.partial(place_kernel, len(mine)),
        in_specs=[smem] + [vmem] * len(pieces),
        out_specs=hbm,
        out_shape=jax.ShapeDtypeStruct((rows, width), bf16),
        scratch_shapes=[pltpu.SemaphoreType.DMA((len(pieces),))],
        compiler_params=room(6),
        cost_estimate=cost(1 << 28),
        name="place",
    )(scalar(core), *pieces)


def local(tokens, forget, attn_gain, projections, out_weight, ffn_gain, expand_weight, down_weight):
    row_count, width = tokens.shape
    head_count = forget.shape[1]
    head_size = projections.shape[2] // head_count
    chips = lax.axis_size("tp") // cores
    core = lax.axis_index("tp") % cores
    parity = lax.axis_index("seq") % 2

    far = [across_chips(x) for x in cut_columns(parity, out_weight, 2)]
    out_partner = swap_cores(out_weight)
    expand_other = swap_cores(expand_weight)
    down_other = swap_cores(down_weight)

    k, v, normed, query_weight, column, row, state, sent = project(
        tokens, attn_gain, forget, projections, head_size
    )
    before = incoming_state(state, sent, head_size)
    q = queries(normed, query_weight, head_size)
    parts = 2
    inside = []
    for part in range(parts):
        inside.append(block_attention(q, k, v, column, row, head_size, part, parts))
    kept = finish_heads(core, q, column, before, inside, head_size)
    given = finish_heads(1 - core, q, column, before, inside, head_size)
    moved = swap_cores(given)
    sums, expand_here, expand_other = project_own_heads(
        kept, moved, out_weight, out_partner, expand_weight, expand_other
    )
    for hop in range(1, chips):
        other = [with_seq(x, 1) for x in far]
        weights = [x for value in far + other for x in (value, swap_cores(value))]
        kept, moved = across_chips(kept), across_chips(moved)
        sums = project_far_heads(parity, kept, moved, weights, sums)
        if hop + 1 < chips:
            far = [across_chips(x) for x in far]
    residual, normed_ffn = add_residual(core, tokens, sums, ffn_gain)
    hidden, down_here, down_other = expand(normed_ffn, expand_here, expand_other, down_weight, down_other)
    pieces = 4
    span = width // pieces
    mine, theirs = [], []
    for piece in range(pieces):
        partial = down(hidden, down_here, down_other, piece * span, span)
        moving, others = partial, []
        for _ in range(1, chips):
            moving = across_chips(moving)
            others.append(moving)
        mine.append(add_partials(piece * span, residual, partial, others))
        theirs.append(swap_cores(mine[-1]))
    return place(core, mine, theirs, row_count)


def solution(mesh):
    placed = (
        P("seq", None),
        P("seq", "tp"),
        P(),
        P(None, None, "tp"),
        P("tp", None),
        P(),
        P(None, None, "tp"),
        P("tp", None),
    )
    return jax.shard_map(
        local, mesh=mesh, in_specs=placed, out_specs=P("seq", None), check_vma=False
    )
```

```python
import functools
import math

import jax
import jax.numpy as jnp
from jax import lax
from jax.experimental import pallas as pl
from jax.experimental.pallas import tpu as pltpu
from jax.sharding import PartitionSpec as P

norm_epsilon = 1e-05
head_epsilon = 1e-06
cores = 2
log2e = 1.4426950408889634

f32, bf16 = jnp.float32, jnp.bfloat16
chunks = 2
spans = ((1,), (2, 4, 4))


vmem = pl.BlockSpec(memory_space=pltpu.VMEM)
hbm = pl.BlockSpec(memory_space=pltpu.HBM)


def cost(flops):
    return pl.CostEstimate(flops=flops, bytes_accessed=0, transcendentals=0)


def room(mebibytes):
    return pltpu.CompilerParams(vmem_limit_bytes=mebibytes << 20)


def own_core():
    return lax.axis_index("tp") % cores


def iota(shape, axis):
    return lax.broadcasted_iota(jnp.int32, shape, axis)


def dot(a, b):
    return jnp.dot(a, b, preferred_element_type=f32)


def contract(a, b, dim_a, dim_b):
    return lax.dot_general(a, b, (((dim_a,), (dim_b,)), ((), ())), preferred_element_type=f32)


def split3(value):
    high = value.astype(bf16)
    rest = value - high.astype(f32)
    middle = rest.astype(bf16)
    return high, middle, (rest - middle.astype(f32)).astype(bf16)


def normalize(rows, gain):
    mean_square = jnp.mean(rows * rows, axis=-1, keepdims=True)
    return (rows * lax.rsqrt(mean_square + norm_epsilon) * gain).astype(bf16)


def spread_heads(sums, size):
    heads = sums.shape[1]
    spread = (iota((heads, heads * size), 1) // size == iota((heads, heads * size), 0)).astype(bf16)
    parts = split3(sums)
    return dot(parts[0], spread) + dot(parts[1], spread) + dot(parts[2], spread)


def swap_cores(value):
    count = lax.axis_size("tp")
    return lax.ppermute(value, "tp", [(i, i ^ 1) for i in range(count)])


def across_chips(value):
    count = lax.axis_size("tp")
    return lax.ppermute(value, "tp", [(i, (i + cores) % count) for i in range(count)])


def with_seq(value, bit):
    count = lax.axis_size("seq")
    return lax.ppermute(value, "seq", [(i, i ^ bit) for i in range(count)])


def project_kernel(
    size, tok, gain, forget, weight, keys, values, normed, query_weight, column, row, state, sent, tok_here, weight_here, sems
):
    heads, rows = forget.shape
    parts = 4
    span = rows // parts
    loads = [
        pltpu.make_async_copy(tok.at[pl.ds(p * span, span)], tok_here.at[pl.ds(p * span, span)], sems.at[p])
        for p in range(parts)
    ]
    for which in (1, 2):
        loads.append(pltpu.make_async_copy(weight.at[which], weight_here.at[which - 1], sems.at[parts + which - 1]))
    loads.append(pltpu.make_async_copy(weight.at[0], query_weight, sems.at[parts + 2]))
    for load in loads:
        load.start()

    pieces = split3(forget[...])
    upper = (iota((rows, rows), 0) <= iota((rows, rows), 1)).astype(bf16)
    sums = (dot(pieces[0], upper) + dot(pieces[1], upper) + dot(pieces[2], upper)) * log2e
    row[...] = sums
    by_token = jnp.transpose(sums)
    column[...] = by_token
    grown = spread_heads(by_token, size)
    ends = grown[rows - 1 :, :]
    decays = jnp.exp2(ends)

    for p in range(parts):
        loads[p].wait()
        here = pl.ds(p * span, span)
        normed[here, :] = normalize(tok_here[here, :].astype(f32), gain[...])
    loads[parts].wait()
    keys[...] = dot(normed[...], weight_here[0]).astype(bf16)
    loads[parts + 1].wait()
    values[...] = dot(normed[...], weight_here[1]).astype(bf16)

    lanes = 2 * size
    first = iota((size, lanes), 1) < size
    picked = jnp.zeros((16, lanes), f32)
    for pair in range(heads // 2):
        cut = slice(pair * lanes, (pair + 1) * lanes)
        shrink = jnp.exp2(ends[:, cut] - grown[:, cut])
        scaled = (keys[:, cut].astype(f32) * shrink).astype(bf16)
        both = contract(scaled, values[:, cut], 0, 0)
        compact = jnp.where(first, both[:size], both[size:])
        state[pl.ds(pair * size, size), :] = compact
        sent[pl.ds(pair * size, size), :] = compact.astype(bf16)
        picked = jnp.where(iota((16, lanes), 0) == pair, jnp.broadcast_to(decays[:, cut], (16, lanes)), picked)
    base = heads // 2 * size
    state[pl.ds(base, 16), :] = picked
    sent[pl.ds(base, 16), :] = picked.astype(bf16)
    loads[parts + 2].wait()


def project(tokens, gain, forget, projections, size):
    rows, width = tokens.shape
    heads = forget.shape[1]
    mine = projections.shape[2]
    packed = (heads // 2 * size + 16, 2 * size)
    outs = [
        ((rows, mine), bf16),
        ((rows, mine), bf16),
        ((rows, width), bf16),
        ((width, mine), bf16),
        ((rows, heads), f32),
        ((heads, rows), f32),
        (packed, f32),
        (packed, bf16),
    ]
    return pl.pallas_call(
        functools.partial(project_kernel, size),
        in_specs=[hbm, vmem, vmem, hbm],
        out_specs=[vmem] * len(outs),
        out_shape=[jax.ShapeDtypeStruct(shape, kind) for shape, kind in outs],
        scratch_shapes=[
            pltpu.VMEM((rows, width), bf16),
            pltpu.VMEM((2, width, mine), bf16),
            pltpu.SemaphoreType.DMA((7,)),
        ],
        cost_estimate=cost(4 * rows * width * mine),
        compiler_params=room(42),
        name="project",
    )(tokens, gain.reshape(1, width), forget.T, projections)


def query_kernel(scale, normed, weight, out):
    out[...] = (dot(normed[...], weight[...]).astype(bf16).astype(f32) * scale).astype(bf16)


def queries(normed, weight, size):
    rows, width = normed.shape
    mine = weight.shape[1]
    return pl.pallas_call(
        functools.partial(query_kernel, 1.0 / math.sqrt(size)),
        in_specs=[vmem] * 2,
        out_specs=vmem,
        out_shape=jax.ShapeDtypeStruct((rows, mine), bf16),
        cost_estimate=cost(2 * rows * width * mine),
        compiler_params=room(8),
        name="queries",
    )(normed, weight)


def block_kernel(size, first_pair, pairs, q, k, v, column, row, out):
    rows, lanes = q.shape[0], 2 * size
    span = rows // 2
    below = iota((span, span), 0) >= iota((span, span), 1)
    for at in range(pairs):
        cut = slice((first_pair + at) * lanes, (first_pair + at + 1) * lanes)
        total = [None, None]
        for side in range(2):
            head = 2 * (first_pair + at) + side
            half = (iota((span, lanes), 1) // size) == side
            zero = jnp.zeros((span, lanes), bf16)
            ks = [jnp.where(half, k[pl.ds(b * span, span), cut], zero) for b in range(2)]
            vs = [jnp.where(half, v[pl.ds(b * span, span), cut], zero) for b in range(2)]
            for tb in range(2):
                here = column[pl.ds(tb * span, span), head : head + 1]
                for sb in range(tb + 1):
                    scores = contract(q[pl.ds(tb * span, span), cut], ks[sb], 1, 1)
                    gap = here - row[head : head + 1, pl.ds(sb * span, span)]
                    if sb == tb:
                        gap = jnp.where(below, gap, -jnp.inf)
                    weights = (scores * jnp.exp2(gap)).astype(bf16)
                    part = dot(weights, vs[sb])
                    total[tb] = part if total[tb] is None else total[tb] + part
        for tb in range(2):
            out[pl.ds(tb * span, span), pl.ds(at * lanes, lanes)] = total[tb]


def block_attention(q, k, v, column, row, size, part, parts):
    rows, mine = q.shape
    heads = column.shape[1]
    wide = mine // parts
    first_pair = part * (heads // 2 // parts)
    return pl.pallas_call(
        functools.partial(block_kernel, size, first_pair, heads // 2 // parts),
        in_specs=[vmem] * 5,
        out_specs=vmem,
        out_shape=jax.ShapeDtypeStruct((rows, wide), f32),
        cost_estimate=cost(16 * rows * rows * wide),
        compiler_params=room(10),
    )(q, k, v, column, row)


def combine_kernel(bit, size, state, before, got, new_before, *carried):
    tail = 16
    body, lanes = state.shape[0] - tail, state.shape[1]
    is_later, first = (lax.axis_index("seq") & bit) != 0, bit == 1
    rest = pl.ds(body, tail)
    mine_decay, got_decay = state[rest, :], got[rest, :].astype(f32)
    early_decay = jnp.ones((tail, lanes), f32) if first else before[rest, :]
    for pair in range(body // size):
        at = pl.ds(pair * size, size)
        theirs, own = got[at, :].astype(f32), state[at, :]
        prior = jnp.zeros((size, lanes), f32) if first else before[at, :]
        d_mine, d_got, d_early = (x[pair : pair + 1] for x in (mine_decay, got_decay, early_decay))
        if carried:
            fresh = jnp.where(is_later, d_mine * theirs + own, d_got * own + theirs)
            for ref in carried:
                ref[at, :] = fresh.astype(ref.dtype)
        new_before[at, :] = jnp.where(is_later, prior + d_early * theirs, prior)
    decay = mine_decay * got_decay
    for ref in carried:
        ref[rest, :] = decay.astype(ref.dtype)
    new_before[rest, :] = jnp.where(is_later, early_decay * got_decay, early_decay)


def combine(bit, size, last, state, before, got):
    kinds = (f32,) if last else (f32, f32, bf16)
    return pl.pallas_call(
        functools.partial(combine_kernel, bit, size),
        in_specs=[vmem] * 3,
        out_specs=[vmem] * len(kinds),
        out_shape=[jax.ShapeDtypeStruct(state.shape, kind) for kind in kinds],
        compiler_params=room(2),
        cost_estimate=cost(1 << 28),
        name="combine",
    )(state, before, got)


def incoming_state(state, sent, size):
    count = lax.axis_size("seq")
    before, bit = state, 1
    while bit < count:
        got = with_seq(sent, bit)
        before, *carried = combine(bit, size, 2 * bit >= count, state, before, got)
        if carried:
            state, sent = carried
        bit *= 2
    return before


def heads_kernel(size, parts, side, start, q, column, before, *refs):
    locals_, out = refs[:parts], refs[parts]
    span, lanes = out.shape[0], 2 * size
    width = q.shape[1] // parts
    core = own_core() if side == 0 else 1 - own_core()
    here = pl.ds(pl.multiple_of(core * (q.shape[0] // cores) + start, span), span)
    ones = (iota((lanes, lanes), 0) // size == iota((lanes, lanes), 1) // size).astype(bf16)
    first = iota((size, lanes), 1) < size
    growth = jnp.exp2(spread_heads(column[here, :], size))
    for pair in range(q.shape[1] // lanes):
        cut = slice(pair * lanes, (pair + 1) * lanes)
        compact = before[pl.ds(pair * size, size), :]
        upper = jnp.where(first, compact, 0.0).astype(bf16)
        under = jnp.where(first, 0.0, compact).astype(bf16)
        block = jnp.concatenate([upper, under], axis=0)
        carried = dot(q[here, cut], block) * growth[:, cut]
        at = pair * lanes % width
        attended = locals_[pair * lanes // width][here, at : at + lanes] + carried
        square = attended * attended
        high = square.astype(bf16)
        low = (square - high.astype(f32)).astype(bf16)
        mean_square = (dot(high, ones) + dot(low, ones)) * (1.0 / size)
        out[:, cut] = (attended * lax.rsqrt(mean_square + head_epsilon)).astype(bf16)


def finish_heads(side, start, span, q, column, before, local_parts, size):
    mine = q.shape[1]
    return pl.pallas_call(
        functools.partial(heads_kernel, size, len(local_parts), side, start),
        in_specs=[vmem] * (3 + len(local_parts)),
        out_specs=vmem,
        out_shape=jax.ShapeDtypeStruct((span, mine), bf16),
        cost_estimate=cost(span * mine * 2048),
        compiler_params=room(6),
        name="finish_heads",
    )(q, column, before, *local_parts)


def own_heads_kernel(kept, moved, own, partner, out):
    out[...] = (dot(kept[...], own[...]) + dot(moved[...], partner[...])).astype(bf16)


def project_heads(kept, moved, own, partner):
    rows, (depth, width) = kept.shape[0], own.shape
    return pl.pallas_call(
        own_heads_kernel,
        in_specs=[vmem] * 4,
        out_specs=vmem,
        out_shape=jax.ShapeDtypeStruct((rows, width), bf16),
        cost_estimate=cost(4 * rows * depth * width),
        compiler_params=room(8),
        name="project_heads",
    )(kept, moved, own, partner)


def residual_kernel(start, half, tok, gain, own, *refs):
    others, residual, normed = refs[:-2], refs[-2], refs[-1]
    rows = own.shape[0]
    total = own[...].astype(f32)
    for other in others:
        total = total + other[...].astype(f32)
    here = pl.ds(pl.multiple_of(own_core() * half + start, rows), rows)
    total = (tok[here, :].astype(f32) + total).astype(bf16)
    residual[...] = total
    normed[...] = normalize(total.astype(f32), gain[...])


def add_residual(tokens, gain, own, others, start):
    shape = jax.ShapeDtypeStruct(own.shape, bf16)
    return pl.pallas_call(
        functools.partial(residual_kernel, start, tokens.shape[0] // cores),
        in_specs=[vmem] * (3 + len(others)),
        out_specs=[vmem] * 2,
        out_shape=[shape, shape],
        cost_estimate=cost(own.size * 1024),
        compiler_params=room(8),
    )(tokens, gain.reshape(1, -1), own, *others)


def expand_kernel(rows_in, own, other, out):
    hidden = own.shape[2]
    wide = hidden // 2
    for place, weight in enumerate((own, other)):
        for at in range(0, hidden, wide):
            gate = dot(rows_in[...], weight[0, :, at : at + wide])
            up = dot(rows_in[...], weight[1, :, at : at + wide])
            half_gate = 0.5 * gate
            silu = half_gate * jnp.tanh(half_gate) + half_gate
            out[:, pl.ds(place * hidden + at, wide)] = (silu * up).astype(bf16)


def expand(rows_in, own, other):
    rows, width = rows_in.shape
    hidden = own.shape[2]
    return pl.pallas_call(
        expand_kernel,
        in_specs=[vmem] * 3,
        out_specs=vmem,
        out_shape=jax.ShapeDtypeStruct((rows, 2 * hidden), bf16),
        cost_estimate=cost(8 * rows * width * hidden),
        compiler_params=room(10),
        name="expand",
    )(rows_in, own, other)


def down_kernel(start, hidden, own, other, out):
    depth, span = own.shape[0], out.shape[1]
    cut = slice(start, start + span)
    out[...] = (dot(hidden[:, :depth], own[:, cut]) + dot(hidden[:, depth:], other[:, cut])).astype(bf16)


def down(hidden, own, other, start, span):
    rows, depth = hidden.shape
    return pl.pallas_call(
        functools.partial(down_kernel, start),
        in_specs=[vmem] * 3,
        out_specs=vmem,
        out_shape=jax.ShapeDtypeStruct((rows, span), bf16),
        cost_estimate=cost(2 * rows * depth * span),
        compiler_params=room(14),
    )(hidden, own, other)


def add_kernel(start, residual, own, *refs):
    out = refs[-1]
    total = own[...].astype(f32)
    for other in refs[:-1]:
        total = total + other[...].astype(f32)
    out[...] = (residual[:, start : start + out.shape[1]].astype(f32) + total).astype(bf16)


def add_partials(start, residual, own, others):
    return pl.pallas_call(
        functools.partial(add_kernel, start),
        in_specs=[vmem] * (2 + len(others)),
        out_specs=vmem,
        out_shape=jax.ShapeDtypeStruct(own.shape, bf16),
        compiler_params=room(4),
        cost_estimate=cost(1 << 28),
        name="add_partials",
    )(residual, own, *others)


def place_kernel(spots, half, *refs):
    pieces, out, sems = refs[: 2 * len(spots)], refs[-2], refs[-1]
    loads = []
    for at, (row, column) in enumerate(spots):
        rows, columns = pieces[2 * at].shape
        for side in range(2):
            core = own_core() if side == 0 else 1 - own_core()
            here = pl.ds(pl.multiple_of(core * half + row, rows), rows)
            to = out.at[here, pl.ds(column, columns)]
            loads.append(pltpu.make_async_copy(pieces[2 * at + side], to, sems.at[2 * at + side]))
    for load in loads:
        load.start()
    for load in loads:
        load.wait()


def place(mine, theirs, spots, shape, target=None):
    pieces = [x for pair in zip(mine, theirs) for x in pair]
    given = [] if target is None else [target]
    return pl.pallas_call(
        functools.partial(place_kernel, spots, shape[0] // cores),
        in_specs=[vmem] * len(pieces) + [hbm] * len(given),
        out_specs=hbm,
        out_shape=jax.ShapeDtypeStruct(shape, bf16),
        input_output_aliases={len(pieces): 0} if given else {},
        scratch_shapes=[pltpu.SemaphoreType.DMA((len(pieces),))],
        compiler_params=room(6),
        cost_estimate=cost(1 << 28),
        name="place",
    )(*pieces, *given)


def local(tokens, forget, attn_gain, projections, out_weight, ffn_gain, expand_weight, down_weight):
    row_count, width = tokens.shape
    head_count = forget.shape[1]
    head_size = projections.shape[2] // head_count
    chips = lax.axis_size("tp") // cores

    half = row_count // cores
    expand_other = swap_cores(expand_weight)
    out_partner = swap_cores(out_weight)
    down_other = swap_cores(down_weight)

    k, v, normed, query_weight, column, row, state, sent = project(
        tokens, attn_gain, forget, projections, head_size
    )
    before = incoming_state(state, sent, head_size)
    q = queries(normed, query_weight, head_size)
    parts = 2
    inside = []
    for part in range(parts):
        inside.append(block_attention(q, k, v, column, row, head_size, part, parts))
    def exchanged(value):
        others = []
        for _ in range(1, chips):
            value = across_chips(value)
            others.append(value)
        return others

    chunk = half // chunks
    sums = []
    for at in range(chunks):
        given = finish_heads(1, at * chunk, chunk, q, column, before, inside, head_size)
        kept = finish_heads(0, at * chunk, chunk, q, column, before, inside, head_size)
        moved = swap_cores(given)
        part = project_heads(kept, moved, out_weight, out_partner)
        sums.append((part, exchanged(part)))
    mine, theirs, spots = [], [], []
    for at, (part, others) in enumerate(sums):
        residual, normed_ffn = add_residual(tokens, ffn_gain, part, others, at * chunk)
        hidden = expand(normed_ffn, expand_weight, expand_other)
        start = 0
        for parts_of in spans[at]:
            span = width // parts_of
            partial = down(hidden, down_weight, down_other, start, span)
            others = exchanged(partial)
            mine.append(add_partials(start, residual, partial, others))
            theirs.append(swap_cores(mine[-1]))
            spots.append((at * chunk, start))
            start += span
    late = 2
    output = place(mine[:-late], theirs[:-late], spots[:-late], tokens.shape)
    return place(mine[-late:], theirs[-late:], spots[-late:], tokens.shape, output)


def solution(mesh):
    placed = (
        P("seq", None),
        P("seq", "tp"),
        P(),
        P(None, None, "tp"),
        P("tp", None),
        P(),
        P(None, None, "tp"),
        P("tp", None),
    )
    return jax.shard_map(
        local, mesh=mesh, in_specs=placed, out_specs=P("seq", None), check_vma=False
    )
```

```python
import functools
import math

import jax
import jax.numpy as jnp
from jax import lax
from jax.experimental import pallas as pl
from jax.experimental.pallas import tpu as pltpu
from jax.sharding import PartitionSpec as P

norm_epsilon = 1e-05
head_epsilon = 1e-06
cores = 2
log2e = 1.4426950408889634

f32, bf16 = jnp.float32, jnp.bfloat16
chunks = 2
spans = ((1,), (2, 4, 4))


vmem = pl.BlockSpec(memory_space=pltpu.VMEM)
hbm = pl.BlockSpec(memory_space=pltpu.HBM)


def cost(flops):
    return pl.CostEstimate(flops=flops, bytes_accessed=0, transcendentals=0)


def room(mebibytes):
    return pltpu.CompilerParams(vmem_limit_bytes=mebibytes << 20)


def own_core():
    return lax.axis_index("tp") % cores


def iota(shape, axis):
    return lax.broadcasted_iota(jnp.int32, shape, axis)


def dot(a, b):
    return jnp.dot(a, b, preferred_element_type=f32)


def contract(a, b, dim_a, dim_b):
    return lax.dot_general(a, b, (((dim_a,), (dim_b,)), ((), ())), preferred_element_type=f32)


def split3(value):
    high = value.astype(bf16)
    rest = value - high.astype(f32)
    middle = rest.astype(bf16)
    return high, middle, (rest - middle.astype(f32)).astype(bf16)


def normalize(rows, gain):
    mean_square = jnp.mean(rows * rows, axis=-1, keepdims=True)
    return (rows * lax.rsqrt(mean_square + norm_epsilon) * gain).astype(bf16)


def spread_heads(sums, size):
    heads = sums.shape[1]
    spread = (iota((heads, heads * size), 1) // size == iota((heads, heads * size), 0)).astype(bf16)
    parts = split3(sums)
    return dot(parts[0], spread) + dot(parts[1], spread) + dot(parts[2], spread)


def swap_cores(value):
    count = lax.axis_size("tp")
    return lax.ppermute(value, "tp", [(i, i ^ 1) for i in range(count)])


def across_chips(value):
    count = lax.axis_size("tp")
    return lax.ppermute(value, "tp", [(i, (i + cores) % count) for i in range(count)])


def with_seq(value, bit):
    count = lax.axis_size("seq")
    return lax.ppermute(value, "seq", [(i, i ^ bit) for i in range(count)])


def project_kernel(
    size, opened, tok, gain, forget, weight, keys, values, normed, query_weight, column, row, state, sent, weight_here, sems
):
    heads, rows = forget.shape
    targets = (weight_here.at[0], weight_here.at[1], query_weight)
    loads = [
        pltpu.make_async_copy(weight.at[which], target, sems.at[at])
        for at, (which, target) in enumerate(zip((1, 2, 0), targets))
    ]
    for load in loads:
        load.start()

    pieces = split3(forget[...])
    upper = (iota((rows, rows), 0) <= iota((rows, rows), 1)).astype(bf16)
    sums = (dot(pieces[0], upper) + dot(pieces[1], upper) + dot(pieces[2], upper)) * log2e
    row[...] = sums
    by_token = jnp.transpose(sums)
    column[...] = by_token
    grown = spread_heads(by_token, size)
    ends = grown[rows - 1 :, :]
    decays = jnp.exp2(ends)

    normed[...] = normalize(tok[...].astype(f32), gain[...])
    loads[0].wait()
    keys[...] = dot(normed[...], weight_here[0]).astype(bf16)
    loads[1].wait()
    values[...] = dot(normed[...], weight_here[1]).astype(bf16)

    lanes = 2 * size
    first = iota((size, lanes), 1) < size
    picked = jnp.zeros((16, lanes), f32)
    for pair in range(heads // 2):
        cut = slice(pair * lanes, (pair + 1) * lanes)
        shrink = jnp.exp2(ends[:, cut] - grown[:, cut])
        scaled = (keys[:, cut].astype(f32) * shrink).astype(bf16)
        both = contract(scaled, values[:, cut], 0, 0)
        compact = jnp.where(first, both[:size], both[size:])
        state[pl.ds(pair * size, size), :] = compact
        sent[pl.ds(pair * size, size), :] = compact.astype(bf16)
        picked = jnp.where(iota((16, lanes), 0) == pair, jnp.broadcast_to(decays[:, cut], (16, lanes)), picked)
    base = heads // 2 * size
    state[pl.ds(base, 16), :] = picked
    sent[pl.ds(base, 16), :] = picked.astype(bf16)
    loads[2].wait()


def open_kernel(out):
    out[...] = jnp.zeros_like(out)


def opening():
    return pl.pallas_call(
        open_kernel,
        out_specs=vmem,
        out_shape=jax.ShapeDtypeStruct((8, 128), f32),
        compiler_params=room(1),
        cost_estimate=cost(1 << 32),
        name="opening",
    )()


def project(opened, tokens, gain, forget, projections, size):
    rows, width = tokens.shape
    heads = forget.shape[1]
    mine = projections.shape[2]
    packed = (heads // 2 * size + 16, 2 * size)
    outs = [
        ((rows, mine), bf16),
        ((rows, mine), bf16),
        ((rows, width), bf16),
        ((width, mine), bf16),
        ((rows, heads), f32),
        ((heads, rows), f32),
        (packed, f32),
        (packed, bf16),
    ]
    return pl.pallas_call(
        functools.partial(project_kernel, size),
        in_specs=[hbm, vmem, vmem, vmem, hbm],
        out_specs=[vmem] * len(outs),
        out_shape=[jax.ShapeDtypeStruct(shape, kind) for shape, kind in outs],
        scratch_shapes=[
            pltpu.VMEM((2, width, mine), bf16),
            pltpu.SemaphoreType.DMA((3,)),
        ],
        cost_estimate=cost(4 * rows * width * mine),
        compiler_params=room(42),
        name="project",
    )(opened, tokens, gain.reshape(1, width), forget.T, projections)


def query_kernel(scale, normed, weight, out):
    out[...] = (dot(normed[...], weight[...]).astype(bf16).astype(f32) * scale).astype(bf16)


def queries(normed, weight, size):
    rows, width = normed.shape
    mine = weight.shape[1]
    return pl.pallas_call(
        functools.partial(query_kernel, 1.0 / math.sqrt(size)),
        in_specs=[vmem] * 2,
        out_specs=vmem,
        out_shape=jax.ShapeDtypeStruct((rows, mine), bf16),
        cost_estimate=cost(2 * rows * width * mine),
        compiler_params=room(8),
        name="queries",
    )(normed, weight)


def block_kernel(size, first_pair, pairs, q, k, v, column, row, out):
    rows, lanes = q.shape[0], 2 * size
    span = rows // 2
    below = iota((span, span), 0) >= iota((span, span), 1)
    for at in range(pairs):
        cut = slice((first_pair + at) * lanes, (first_pair + at + 1) * lanes)
        total = [None, None]
        for side in range(2):
            head = 2 * (first_pair + at) + side
            half = (iota((span, lanes), 1) // size) == side
            zero = jnp.zeros((span, lanes), bf16)
            ks = [jnp.where(half, k[pl.ds(b * span, span), cut], zero) for b in range(2)]
            vs = [jnp.where(half, v[pl.ds(b * span, span), cut], zero) for b in range(2)]
            for tb in range(2):
                here = column[pl.ds(tb * span, span), head : head + 1]
                for sb in range(tb + 1):
                    scores = contract(q[pl.ds(tb * span, span), cut], ks[sb], 1, 1)
                    gap = here - row[head : head + 1, pl.ds(sb * span, span)]
                    if sb == tb:
                        gap = jnp.where(below, gap, -jnp.inf)
                    weights = (scores * jnp.exp2(gap)).astype(bf16)
                    part = dot(weights, vs[sb])
                    total[tb] = part if total[tb] is None else total[tb] + part
        for tb in range(2):
            out[pl.ds(tb * span, span), pl.ds(at * lanes, lanes)] = total[tb]


def block_attention(q, k, v, column, row, size, part, parts):
    rows, mine = q.shape
    heads = column.shape[1]
    wide = mine // parts
    first_pair = part * (heads // 2 // parts)
    return pl.pallas_call(
        functools.partial(block_kernel, size, first_pair, heads // 2 // parts),
        in_specs=[vmem] * 5,
        out_specs=vmem,
        out_shape=jax.ShapeDtypeStruct((rows, wide), f32),
        cost_estimate=cost(16 * rows * rows * wide),
        compiler_params=room(10),
    )(q, k, v, column, row)


def combine_kernel(bit, size, state, before, got, new_before, *carried):
    tail = 16
    body, lanes = state.shape[0] - tail, state.shape[1]
    is_later, first = (lax.axis_index("seq") & bit) != 0, bit == 1
    rest = pl.ds(body, tail)
    mine_decay, got_decay = state[rest, :], got[rest, :].astype(f32)
    early_decay = jnp.ones((tail, lanes), f32) if first else before[rest, :]
    for pair in range(body // size):
        at = pl.ds(pair * size, size)
        theirs, own = got[at, :].astype(f32), state[at, :]
        prior = jnp.zeros((size, lanes), f32) if first else before[at, :]
        d_mine, d_got, d_early = (x[pair : pair + 1] for x in (mine_decay, got_decay, early_decay))
        if carried:
            fresh = jnp.where(is_later, d_mine * theirs + own, d_got * own + theirs)
            for ref in carried:
                ref[at, :] = fresh.astype(ref.dtype)
        new_before[at, :] = jnp.where(is_later, prior + d_early * theirs, prior)
    decay = mine_decay * got_decay
    for ref in carried:
        ref[rest, :] = decay.astype(ref.dtype)
    new_before[rest, :] = jnp.where(is_later, early_decay * got_decay, early_decay)


def combine(bit, size, last, state, before, got):
    kinds = (f32,) if last else (f32, f32, bf16)
    return pl.pallas_call(
        functools.partial(combine_kernel, bit, size),
        in_specs=[vmem] * 3,
        out_specs=[vmem] * len(kinds),
        out_shape=[jax.ShapeDtypeStruct(state.shape, kind) for kind in kinds],
        compiler_params=room(2),
        cost_estimate=cost(1 << 28),
        name="combine",
    )(state, before, got)


def incoming_state(state, sent, size):
    count = lax.axis_size("seq")
    before, bit = state, 1
    while bit < count:
        got = with_seq(sent, bit)
        before, *carried = combine(bit, size, 2 * bit >= count, state, before, got)
        if carried:
            state, sent = carried
        bit *= 2
    return before


def heads_kernel(size, parts, side, start, q, column, before, *refs):
    locals_, out = refs[:parts], refs[parts]
    span, lanes = out.shape[0], 2 * size
    width = q.shape[1] // parts
    core = own_core() if side == 0 else 1 - own_core()
    here = pl.ds(pl.multiple_of(core * (q.shape[0] // cores) + start, span), span)
    ones = (iota((lanes, lanes), 0) // size == iota((lanes, lanes), 1) // size).astype(bf16)
    first = iota((size, lanes), 1) < size
    growth = jnp.exp2(spread_heads(column[here, :], size))
    for pair in range(q.shape[1] // lanes):
        cut = slice(pair * lanes, (pair + 1) * lanes)
        compact = before[pl.ds(pair * size, size), :]
        upper = jnp.where(first, compact, 0.0).astype(bf16)
        under = jnp.where(first, 0.0, compact).astype(bf16)
        block = jnp.concatenate([upper, under], axis=0)
        carried = dot(q[here, cut], block) * growth[:, cut]
        at = pair * lanes % width
        attended = locals_[pair * lanes // width][here, at : at + lanes] + carried
        square = attended * attended
        high = square.astype(bf16)
        low = (square - high.astype(f32)).astype(bf16)
        mean_square = (dot(high, ones) + dot(low, ones)) * (1.0 / size)
        out[:, cut] = (attended * lax.rsqrt(mean_square + head_epsilon)).astype(bf16)


def finish_heads(side, start, span, q, column, before, local_parts, size):
    mine = q.shape[1]
    return pl.pallas_call(
        functools.partial(heads_kernel, size, len(local_parts), side, start),
        in_specs=[vmem] * (3 + len(local_parts)),
        out_specs=vmem,
        out_shape=jax.ShapeDtypeStruct((span, mine), bf16),
        cost_estimate=cost(span * mine * 2048),
        compiler_params=room(6),
        name="finish_heads",
    )(q, column, before, *local_parts)


def own_heads_kernel(kept, moved, own, partner, out):
    out[...] = (dot(kept[...], own[...]) + dot(moved[...], partner[...])).astype(bf16)


def project_heads(kept, moved, own, partner):
    rows, (depth, width) = kept.shape[0], own.shape
    return pl.pallas_call(
        own_heads_kernel,
        in_specs=[vmem] * 4,
        out_specs=vmem,
        out_shape=jax.ShapeDtypeStruct((rows, width), bf16),
        cost_estimate=cost(4 * rows * depth * width),
        compiler_params=room(8),
        name="project_heads",
    )(kept, moved, own, partner)


def residual_kernel(start, half, tok, gain, own, *refs):
    others, residual, normed = refs[:-2], refs[-2], refs[-1]
    rows = own.shape[0]
    total = own[...].astype(f32)
    for other in others:
        total = total + other[...].astype(f32)
    here = pl.ds(pl.multiple_of(own_core() * half + start, rows), rows)
    total = (tok[here, :].astype(f32) + total).astype(bf16)
    residual[...] = total
    normed[...] = normalize(total.astype(f32), gain[...])


def add_residual(tokens, gain, own, others, start):
    shape = jax.ShapeDtypeStruct(own.shape, bf16)
    return pl.pallas_call(
        functools.partial(residual_kernel, start, tokens.shape[0] // cores),
        in_specs=[vmem] * (3 + len(others)),
        out_specs=[vmem] * 2,
        out_shape=[shape, shape],
        cost_estimate=cost(own.size * 1024),
        compiler_params=room(8),
    )(tokens, gain.reshape(1, -1), own, *others)


def expand_kernel(rows_in, own, other, out):
    hidden = own.shape[2]
    wide = hidden // 2
    for place, weight in enumerate((own, other)):
        for at in range(0, hidden, wide):
            gate = dot(rows_in[...], weight[0, :, at : at + wide])
            up = dot(rows_in[...], weight[1, :, at : at + wide])
            half_gate = 0.5 * gate
            silu = half_gate * jnp.tanh(half_gate) + half_gate
            out[:, pl.ds(place * hidden + at, wide)] = (silu * up).astype(bf16)


def expand(rows_in, own, other):
    rows, width = rows_in.shape
    hidden = own.shape[2]
    return pl.pallas_call(
        expand_kernel,
        in_specs=[vmem] * 3,
        out_specs=vmem,
        out_shape=jax.ShapeDtypeStruct((rows, 2 * hidden), bf16),
        cost_estimate=cost(8 * rows * width * hidden),
        compiler_params=room(10),
        name="expand",
    )(rows_in, own, other)


def down_kernel(start, hidden, own, other, out):
    depth, span = own.shape[0], out.shape[1]
    cut = slice(start, start + span)
    out[...] = (dot(hidden[:, :depth], own[:, cut]) + dot(hidden[:, depth:], other[:, cut])).astype(bf16)


def down(hidden, own, other, start, span):
    rows, depth = hidden.shape
    return pl.pallas_call(
        functools.partial(down_kernel, start),
        in_specs=[vmem] * 3,
        out_specs=vmem,
        out_shape=jax.ShapeDtypeStruct((rows, span), bf16),
        cost_estimate=cost(2 * rows * depth * span),
        compiler_params=room(14),
    )(hidden, own, other)


def add_kernel(start, residual, own, *refs):
    out = refs[-1]
    total = own[...].astype(f32)
    for other in refs[:-1]:
        total = total + other[...].astype(f32)
    out[...] = (residual[:, start : start + out.shape[1]].astype(f32) + total).astype(bf16)


def add_partials(start, residual, own, others):
    return pl.pallas_call(
        functools.partial(add_kernel, start),
        in_specs=[vmem] * (2 + len(others)),
        out_specs=vmem,
        out_shape=jax.ShapeDtypeStruct(own.shape, bf16),
        compiler_params=room(4),
        cost_estimate=cost(1 << 28),
        name="add_partials",
    )(residual, own, *others)


def place_kernel(spots, half, *refs):
    pieces, out, sems = refs[: 2 * len(spots)], refs[-2], refs[-1]
    loads = []
    for at, (row, column) in enumerate(spots):
        rows, columns = pieces[2 * at].shape
        for side in range(2):
            core = own_core() if side == 0 else 1 - own_core()
            here = pl.ds(pl.multiple_of(core * half + row, rows), rows)
            to = out.at[here, pl.ds(column, columns)]
            loads.append(pltpu.make_async_copy(pieces[2 * at + side], to, sems.at[2 * at + side]))
    for load in loads:
        load.start()
    for load in loads:
        load.wait()


def place(mine, theirs, spots, shape, target=None):
    pieces = [x for pair in zip(mine, theirs) for x in pair]
    given = [] if target is None else [target]
    return pl.pallas_call(
        functools.partial(place_kernel, spots, shape[0] // cores),
        in_specs=[vmem] * len(pieces) + [hbm] * len(given),
        out_specs=hbm,
        out_shape=jax.ShapeDtypeStruct(shape, bf16),
        input_output_aliases={len(pieces): 0} if given else {},
        scratch_shapes=[pltpu.SemaphoreType.DMA((len(pieces),))],
        compiler_params=room(6),
        cost_estimate=cost(1 << 28),
        name="place",
    )(*pieces, *given)


def local(tokens, forget, attn_gain, projections, out_weight, ffn_gain, expand_weight, down_weight):
    row_count, width = tokens.shape
    head_count = forget.shape[1]
    head_size = projections.shape[2] // head_count
    chips = lax.axis_size("tp") // cores

    half = row_count // cores
    expand_other = swap_cores(expand_weight)
    out_partner = swap_cores(out_weight)
    down_other = swap_cores(down_weight)

    k, v, normed, query_weight, column, row, state, sent = project(
        opening(), tokens, attn_gain, forget, projections, head_size
    )
    before = incoming_state(state, sent, head_size)
    q = queries(normed, query_weight, head_size)
    parts = 2
    inside = []
    for part in range(parts):
        inside.append(block_attention(q, k, v, column, row, head_size, part, parts))
    def exchanged(value):
        others = []
        for _ in range(1, chips):
            value = across_chips(value)
            others.append(value)
        return others

    chunk = half // chunks
    sums = []
    for at in range(chunks):
        given = finish_heads(1, at * chunk, chunk, q, column, before, inside, head_size)
        kept = finish_heads(0, at * chunk, chunk, q, column, before, inside, head_size)
        moved = swap_cores(given)
        part = project_heads(kept, moved, out_weight, out_partner)
        sums.append((part, exchanged(part)))
    mine, theirs, spots = [], [], []
    for at, (part, others) in enumerate(sums):
        residual, normed_ffn = add_residual(tokens, ffn_gain, part, others, at * chunk)
        hidden = expand(normed_ffn, expand_weight, expand_other)
        start = 0
        for parts_of in spans[at]:
            span = width // parts_of
            partial = down(hidden, down_weight, down_other, start, span)
            others = exchanged(partial)
            mine.append(add_partials(start, residual, partial, others))
            theirs.append(swap_cores(mine[-1]))
            spots.append((at * chunk, start))
            start += span
    late = 2
    output = place(mine[:-late], theirs[:-late], spots[:-late], tokens.shape)
    return place(mine[-late:], theirs[-late:], spots[-late:], tokens.shape, output)


def solution(mesh):
    placed = (
        P("seq", None),
        P("seq", "tp"),
        P(),
        P(None, None, "tp"),
        P("tp", None),
        P(),
        P(None, None, "tp"),
        P("tp", None),
    )
    return jax.shard_map(
        local, mesh=mesh, in_specs=placed, out_specs=P("seq", None), check_vma=False
    )
```

```python
import functools
import math

import jax
import jax.numpy as jnp
from jax import lax
from jax.experimental import pallas as pl
from jax.experimental.pallas import tpu as pltpu
from jax.sharding import PartitionSpec as P

norm_epsilon = 1e-05
head_epsilon = 1e-06
cores = 2
log2e = 1.4426950408889634

f32, bf16 = jnp.float32, jnp.bfloat16
chunks = (4, 4, 4, 4)
spans = ((1,), (1,), (1,), (2, 2))


vmem = pl.BlockSpec(memory_space=pltpu.VMEM)
hbm = pl.BlockSpec(memory_space=pltpu.HBM)


def cost(flops):
    return pl.CostEstimate(flops=flops, bytes_accessed=0, transcendentals=0)


def room(mebibytes):
    return pltpu.CompilerParams(vmem_limit_bytes=mebibytes << 20)


def own_core():
    return lax.axis_index("tp") % cores


def iota(shape, axis):
    return lax.broadcasted_iota(jnp.int32, shape, axis)


def dot(a, b):
    return jnp.dot(a, b, preferred_element_type=f32)


def contract(a, b, dim_a, dim_b):
    return lax.dot_general(a, b, (((dim_a,), (dim_b,)), ((), ())), preferred_element_type=f32)


def split3(value):
    high = value.astype(bf16)
    rest = value - high.astype(f32)
    middle = rest.astype(bf16)
    return high, middle, (rest - middle.astype(f32)).astype(bf16)


def normalize(rows, gain):
    mean_square = jnp.mean(rows * rows, axis=-1, keepdims=True)
    return (rows * lax.rsqrt(mean_square + norm_epsilon) * gain).astype(bf16)


def spread_heads(sums, size):
    heads = sums.shape[1]
    spread = (iota((heads, heads * size), 1) // size == iota((heads, heads * size), 0)).astype(bf16)
    parts = split3(sums)
    return dot(parts[0], spread) + dot(parts[1], spread) + dot(parts[2], spread)


def swap_cores(value):
    count = lax.axis_size("tp")
    return lax.ppermute(value, "tp", [(i, i ^ 1) for i in range(count)])


def across_chips(value):
    count = lax.axis_size("tp")
    return lax.ppermute(value, "tp", [(i, (i + cores) % count) for i in range(count)])


def with_seq(value, bit):
    count = lax.axis_size("seq")
    return lax.ppermute(value, "seq", [(i, i ^ bit) for i in range(count)])


def project_kernel(
    size, opened, tok, gain, forget, weight, keys, values, normed, query_weight, column, row, state, sent, weight_here, sems
):
    heads, rows = forget.shape
    targets = (weight_here.at[0], weight_here.at[1], query_weight)
    loads = [
        pltpu.make_async_copy(weight.at[which], target, sems.at[at])
        for at, (which, target) in enumerate(zip((1, 2, 0), targets))
    ]
    for load in loads:
        load.start()

    pieces = split3(forget[...])
    upper = (iota((rows, rows), 0) <= iota((rows, rows), 1)).astype(bf16)
    sums = (dot(pieces[0], upper) + dot(pieces[1], upper) + dot(pieces[2], upper)) * log2e
    row[...] = sums
    by_token = jnp.transpose(sums)
    column[...] = by_token
    grown = spread_heads(by_token, size)
    ends = grown[rows - 1 :, :]
    decays = jnp.exp2(ends)

    normed[...] = normalize(tok[...].astype(f32), gain[...])
    loads[0].wait()
    keys[...] = dot(normed[...], weight_here[0]).astype(bf16)
    loads[1].wait()
    values[...] = dot(normed[...], weight_here[1]).astype(bf16)

    lanes = 2 * size
    first = iota((size, lanes), 1) < size
    picked = jnp.zeros((16, lanes), f32)
    for pair in range(heads // 2):
        cut = slice(pair * lanes, (pair + 1) * lanes)
        shrink = jnp.exp2(ends[:, cut] - grown[:, cut])
        scaled = (keys[:, cut].astype(f32) * shrink).astype(bf16)
        both = contract(scaled, values[:, cut], 0, 0)
        compact = jnp.where(first, both[:size], both[size:])
        state[pl.ds(pair * size, size), :] = compact
        sent[pl.ds(pair * size, size), :] = compact.astype(bf16)
        picked = jnp.where(iota((16, lanes), 0) == pair, jnp.broadcast_to(decays[:, cut], (16, lanes)), picked)
    base = heads // 2 * size
    state[pl.ds(base, 16), :] = picked
    sent[pl.ds(base, 16), :] = picked.astype(bf16)
    loads[2].wait()


def open_kernel(out):
    out[...] = jnp.zeros_like(out)


def opening():
    return pl.pallas_call(
        open_kernel,
        out_specs=vmem,
        out_shape=jax.ShapeDtypeStruct((8, 128), f32),
        compiler_params=room(1),
        cost_estimate=cost(1 << 32),
        name="opening",
    )()


def project(opened, tokens, gain, forget, projections, size):
    rows, width = tokens.shape
    heads = forget.shape[1]
    mine = projections.shape[2]
    packed = (heads // 2 * size + 16, 2 * size)
    outs = [
        ((rows, mine), bf16),
        ((rows, mine), bf16),
        ((rows, width), bf16),
        ((width, mine), bf16),
        ((rows, heads), f32),
        ((heads, rows), f32),
        (packed, f32),
        (packed, bf16),
    ]
    return pl.pallas_call(
        functools.partial(project_kernel, size),
        in_specs=[hbm, vmem, vmem, vmem, hbm],
        out_specs=[vmem] * len(outs),
        out_shape=[jax.ShapeDtypeStruct(shape, kind) for shape, kind in outs],
        scratch_shapes=[
            pltpu.VMEM((2, width, mine), bf16),
            pltpu.SemaphoreType.DMA((3,)),
        ],
        cost_estimate=cost(4 * rows * width * mine),
        compiler_params=room(42),
        name="project",
    )(opened, tokens, gain.reshape(1, width), forget.T, projections)


def query_kernel(scale, normed, weight, out):
    out[...] = (dot(normed[...], weight[...]).astype(bf16).astype(f32) * scale).astype(bf16)


def queries(normed, weight, size):
    rows, width = normed.shape
    mine = weight.shape[1]
    return pl.pallas_call(
        functools.partial(query_kernel, 1.0 / math.sqrt(size)),
        in_specs=[vmem] * 2,
        out_specs=vmem,
        out_shape=jax.ShapeDtypeStruct((rows, mine), bf16),
        cost_estimate=cost(2 * rows * width * mine),
        compiler_params=room(8),
        name="queries",
    )(normed, weight)


def block_kernel(size, first_pair, pairs, q, k, v, column, row, out):
    rows, lanes = q.shape[0], 2 * size
    span = rows // 2
    below = iota((span, span), 0) >= iota((span, span), 1)
    for at in range(pairs):
        cut = slice((first_pair + at) * lanes, (first_pair + at + 1) * lanes)
        total = [None, None]
        for side in range(2):
            head = 2 * (first_pair + at) + side
            half = (iota((span, lanes), 1) // size) == side
            zero = jnp.zeros((span, lanes), bf16)
            ks = [jnp.where(half, k[pl.ds(b * span, span), cut], zero) for b in range(2)]
            vs = [jnp.where(half, v[pl.ds(b * span, span), cut], zero) for b in range(2)]
            for tb in range(2):
                here = column[pl.ds(tb * span, span), head : head + 1]
                for sb in range(tb + 1):
                    scores = contract(q[pl.ds(tb * span, span), cut], ks[sb], 1, 1)
                    gap = here - row[head : head + 1, pl.ds(sb * span, span)]
                    if sb == tb:
                        gap = jnp.where(below, gap, -jnp.inf)
                    weights = (scores * jnp.exp2(gap)).astype(bf16)
                    part = dot(weights, vs[sb])
                    total[tb] = part if total[tb] is None else total[tb] + part
        for tb in range(2):
            out[pl.ds(tb * span, span), pl.ds(at * lanes, lanes)] = total[tb]


def block_attention(q, k, v, column, row, size, part, parts):
    rows, mine = q.shape
    heads = column.shape[1]
    wide = mine // parts
    first_pair = part * (heads // 2 // parts)
    return pl.pallas_call(
        functools.partial(block_kernel, size, first_pair, heads // 2 // parts),
        in_specs=[vmem] * 5,
        out_specs=vmem,
        out_shape=jax.ShapeDtypeStruct((rows, wide), f32),
        cost_estimate=cost(16 * rows * rows * wide),
        compiler_params=room(10),
    )(q, k, v, column, row)


def combine_kernel(bit, size, state, before, got, new_before, *carried):
    tail = 16
    body, lanes = state.shape[0] - tail, state.shape[1]
    is_later, first = (lax.axis_index("seq") & bit) != 0, bit == 1
    rest = pl.ds(body, tail)
    mine_decay, got_decay = state[rest, :], got[rest, :].astype(f32)
    early_decay = jnp.ones((tail, lanes), f32) if first else before[rest, :]
    for pair in range(body // size):
        at = pl.ds(pair * size, size)
        theirs, own = got[at, :].astype(f32), state[at, :]
        prior = jnp.zeros((size, lanes), f32) if first else before[at, :]
        d_mine, d_got, d_early = (x[pair : pair + 1] for x in (mine_decay, got_decay, early_decay))
        if carried:
            fresh = jnp.where(is_later, d_mine * theirs + own, d_got * own + theirs)
            for ref in carried:
                ref[at, :] = fresh.astype(ref.dtype)
        new_before[at, :] = jnp.where(is_later, prior + d_early * theirs, prior)
    decay = mine_decay * got_decay
    for ref in carried:
        ref[rest, :] = decay.astype(ref.dtype)
    new_before[rest, :] = jnp.where(is_later, early_decay * got_decay, early_decay)


def combine(bit, size, last, state, before, got):
    kinds = (f32,) if last else (f32, f32, bf16)
    return pl.pallas_call(
        functools.partial(combine_kernel, bit, size),
        in_specs=[vmem] * 3,
        out_specs=[vmem] * len(kinds),
        out_shape=[jax.ShapeDtypeStruct(state.shape, kind) for kind in kinds],
        compiler_params=room(2),
        cost_estimate=cost(1 << 28),
        name="combine",
    )(state, before, got)


def incoming_state(state, sent, size):
    count = lax.axis_size("seq")
    before, bit = state, 1
    while bit < count:
        got = with_seq(sent, bit)
        before, *carried = combine(bit, size, 2 * bit >= count, state, before, got)
        if carried:
            state, sent = carried
        bit *= 2
    return before


def heads_kernel(size, parts, side, start, q, column, before, *refs):
    locals_, out = refs[:parts], refs[-1]
    span, lanes = out.shape[0], 2 * size
    width = q.shape[1] // parts
    core = own_core() if side == 0 else 1 - own_core()
    here = pl.ds(pl.multiple_of(core * (q.shape[0] // cores) + start, 16), span)
    ones = (iota((lanes, lanes), 0) // size == iota((lanes, lanes), 1) // size).astype(bf16)
    first = iota((size, lanes), 1) < size
    growth = jnp.exp2(spread_heads(column[here, :], size))
    for pair in range(q.shape[1] // lanes):
        cut = slice(pair * lanes, (pair + 1) * lanes)
        compact = before[pl.ds(pair * size, size), :]
        upper = jnp.where(first, compact, 0.0).astype(bf16)
        under = jnp.where(first, 0.0, compact).astype(bf16)
        block = jnp.concatenate([upper, under], axis=0)
        carried = dot(q[here, cut], block) * growth[:, cut]
        at = pair * lanes % width
        attended = locals_[pair * lanes // width][here, at : at + lanes] + carried
        square = attended * attended
        high = square.astype(bf16)
        low = (square - high.astype(f32)).astype(bf16)
        mean_square = (dot(high, ones) + dot(low, ones)) * (1.0 / size)
        out[:, cut] = (attended * lax.rsqrt(mean_square + head_epsilon)).astype(bf16)
    if len(refs) > parts + 1:
        weight, sums = refs[parts], refs[parts + 1]
        sums[...] = dot(out[...], weight[...])


def finish_heads(side, start, span, q, column, before, local_parts, size):
    mine = q.shape[1]
    return pl.pallas_call(
        functools.partial(heads_kernel, size, len(local_parts), side, start),
        in_specs=[vmem] * (3 + len(local_parts)),
        out_specs=vmem,
        out_shape=jax.ShapeDtypeStruct((span, mine), bf16),
        cost_estimate=cost(span * mine * 2048),
        compiler_params=room(6),
        name="finish_heads",
    )(q, column, before, *local_parts)


def finish_own_heads(start, span, q, column, before, local_parts, weight, size):
    mine, width = weight.shape
    return pl.pallas_call(
        functools.partial(heads_kernel, size, len(local_parts), 0, start),
        in_specs=[vmem] * (4 + len(local_parts)),
        out_specs=vmem,
        out_shape=jax.ShapeDtypeStruct((span, width), f32),
        scratch_shapes=[pltpu.VMEM((span, mine), bf16)],
        cost_estimate=cost(span * mine * 4096),
        compiler_params=room(8),
        name="finish_own_heads",
    )(q, column, before, *local_parts, weight)


def add_heads_kernel(sums, moved, partner, out):
    out[...] = (sums[...] + dot(moved[...], partner[...])).astype(bf16)


def add_heads(sums, moved, partner):
    return pl.pallas_call(
        add_heads_kernel,
        in_specs=[vmem] * 3,
        out_specs=vmem,
        out_shape=jax.ShapeDtypeStruct(sums.shape, bf16),
        cost_estimate=cost(2 * moved.size * sums.shape[1]),
        compiler_params=room(6),
        name="add_heads",
    )(sums, moved, partner)


def residual_kernel(start, half, tok, gain, own, *refs):
    others, residual, normed = refs[:-2], refs[-2], refs[-1]
    rows = own.shape[0]
    total = own[...].astype(f32)
    for other in others:
        total = total + other[...].astype(f32)
    here = pl.ds(pl.multiple_of(own_core() * half + start, 16), rows)
    total = (tok[here, :].astype(f32) + total).astype(bf16)
    residual[...] = total
    normed[...] = normalize(total.astype(f32), gain[...])


def add_residual(tokens, gain, own, others, start):
    shape = jax.ShapeDtypeStruct(own.shape, bf16)
    return pl.pallas_call(
        functools.partial(residual_kernel, start, tokens.shape[0] // cores),
        in_specs=[vmem] * (3 + len(others)),
        out_specs=[vmem] * 2,
        out_shape=[shape, shape],
        cost_estimate=cost(own.size * 1024),
        compiler_params=room(8),
    )(tokens, gain.reshape(1, -1), own, *others)


def expand_kernel(rows_in, own, other, out):
    hidden = own.shape[2]
    wide = hidden // 2
    for place, weight in enumerate((own, other)):
        for at in range(0, hidden, wide):
            gate = dot(rows_in[...], weight[0, :, at : at + wide])
            up = dot(rows_in[...], weight[1, :, at : at + wide])
            half_gate = 0.5 * gate
            silu = half_gate * jnp.tanh(half_gate) + half_gate
            out[:, pl.ds(place * hidden + at, wide)] = (silu * up).astype(bf16)


def expand(rows_in, own, other):
    rows, width = rows_in.shape
    hidden = own.shape[2]
    return pl.pallas_call(
        expand_kernel,
        in_specs=[vmem] * 3,
        out_specs=vmem,
        out_shape=jax.ShapeDtypeStruct((rows, 2 * hidden), bf16),
        cost_estimate=cost(8 * rows * width * hidden),
        compiler_params=room(10),
        name="expand",
    )(rows_in, own, other)


def down_kernel(start, hidden, own, other, out):
    depth, span = own.shape[0], out.shape[1]
    cut = slice(start, start + span)
    out[...] = (dot(hidden[:, :depth], own[:, cut]) + dot(hidden[:, depth:], other[:, cut])).astype(bf16)


def down(hidden, own, other, start, span):
    rows, depth = hidden.shape
    return pl.pallas_call(
        functools.partial(down_kernel, start),
        in_specs=[vmem] * 3,
        out_specs=vmem,
        out_shape=jax.ShapeDtypeStruct((rows, span), bf16),
        cost_estimate=cost(2 * rows * depth * span),
        compiler_params=room(14),
    )(hidden, own, other)


def add_kernel(start, residual, own, *refs):
    out = refs[-1]
    total = own[...].astype(f32)
    for other in refs[:-1]:
        total = total + other[...].astype(f32)
    out[...] = (residual[:, start : start + out.shape[1]].astype(f32) + total).astype(bf16)


def add_partials(start, residual, own, others):
    return pl.pallas_call(
        functools.partial(add_kernel, start),
        in_specs=[vmem] * (2 + len(others)),
        out_specs=vmem,
        out_shape=jax.ShapeDtypeStruct(own.shape, bf16),
        compiler_params=room(4),
        cost_estimate=cost(1 << 28),
        name="add_partials",
    )(residual, own, *others)


def place_kernel(spots, half, *refs):
    pieces, out, sems = refs[: 2 * len(spots)], refs[-2], refs[-1]
    loads = []
    for at, (row, column) in enumerate(spots):
        rows, columns = pieces[2 * at].shape
        for side in range(2):
            core = own_core() if side == 0 else 1 - own_core()
            here = pl.ds(pl.multiple_of(core * half + row, 16), rows)
            to = out.at[here, pl.ds(column, columns)]
            loads.append(pltpu.make_async_copy(pieces[2 * at + side], to, sems.at[2 * at + side]))
    for load in loads:
        load.start()
    for load in loads:
        load.wait()


def place(mine, theirs, spots, shape, target=None):
    pieces = [x for pair in zip(mine, theirs) for x in pair]
    given = [] if target is None else [target]
    return pl.pallas_call(
        functools.partial(place_kernel, spots, shape[0] // cores),
        in_specs=[vmem] * len(pieces) + [hbm] * len(given),
        out_specs=hbm,
        out_shape=jax.ShapeDtypeStruct(shape, bf16),
        input_output_aliases={len(pieces): 0} if given else {},
        scratch_shapes=[pltpu.SemaphoreType.DMA((len(pieces),))],
        compiler_params=room(6),
        cost_estimate=cost(1 << 28),
        name="place",
    )(*pieces, *given)


def local(tokens, forget, attn_gain, projections, out_weight, ffn_gain, expand_weight, down_weight):
    row_count, width = tokens.shape
    head_count = forget.shape[1]
    head_size = projections.shape[2] // head_count
    chips = lax.axis_size("tp") // cores

    half = row_count // cores
    expand_other = swap_cores(expand_weight)
    out_partner = swap_cores(out_weight)
    down_other = swap_cores(down_weight)

    k, v, normed, query_weight, column, row, state, sent = project(
        opening(), tokens, attn_gain, forget, projections, head_size
    )
    before = incoming_state(state, sent, head_size)
    q = queries(normed, query_weight, head_size)
    parts = 2
    inside = []
    for part in range(parts):
        inside.append(block_attention(q, k, v, column, row, head_size, part, parts))
    def exchanged(value):
        others = []
        for _ in range(1, chips):
            value = across_chips(value)
            others.append(value)
        return others

    sizes = [half * share // 16 for share in chunks]
    starts = [sum(sizes[:at]) for at in range(len(sizes))]
    sums = []
    for at, chunk in enumerate(sizes):
        given = finish_heads(1, starts[at], chunk, q, column, before, inside, head_size)
        kept = finish_own_heads(starts[at], chunk, q, column, before, inside, out_weight, head_size)
        moved = swap_cores(given)
        part = add_heads(kept, moved, out_partner)
        sums.append((part, exchanged(part)))
    mine, theirs, spots = [], [], []
    for at, (part, others) in enumerate(sums):
        residual, normed_ffn = add_residual(tokens, ffn_gain, part, others, starts[at])
        hidden = expand(normed_ffn, expand_weight, expand_other)
        start = 0
        for parts_of in spans[at]:
            span = width // parts_of
            partial = down(hidden, down_weight, down_other, start, span)
            others = exchanged(partial)
            mine.append(add_partials(start, residual, partial, others))
            theirs.append(swap_cores(mine[-1]))
            spots.append((starts[at], start))
            start += span
    late = 2
    output = place(mine[:-late], theirs[:-late], spots[:-late], tokens.shape)
    return place(mine[-late:], theirs[-late:], spots[-late:], tokens.shape, output)


def solution(mesh):
    placed = (
        P("seq", None),
        P("seq", "tp"),
        P(),
        P(None, None, "tp"),
        P("tp", None),
        P(),
        P(None, None, "tp"),
        P("tp", None),
    )
    return jax.shard_map(
        local, mesh=mesh, in_specs=placed, out_specs=P("seq", None), check_vma=False
    )
```
